32 devices in a mesh: rep: 2 (over z, core), dp: 16 (over x, y).
Axes of the slice: x: 4, y: 4, z: 1, core: 2. Of those that a mesh axis runs over, the one named last changes fastest.
The devices are a block of a 4x4x8 slice.
Arguments:
- x: bfloat16 [32, 2048, 1024], P(('rep', 'dp')), parts along dimension 0
- dy: bfloat16 [32, 2048, 1024], P(('rep', 'dp')), parts along dimension 0
- w_gate: bfloat16 [2, 1024, 3200], replicated
- w_up: bfloat16 [2, 1024, 3200], replicated
- w_down: bfloat16 [2, 3200, 1024], replicated
- m_w_gate: float32 [2, 1024, 3200], P(None, 'dp')
- m_w_up: float32 [2, 1024, 3200], P(None, 'dp')
- m_w_down: float32 [2, 3200, 1024], P(None, 'dp')
- v_w_gate: float32 [2, 1024, 3200], P(None, 'dp')
- v_w_up: float32 [2, 1024, 3200], P(None, 'dp')
- v_w_down: float32 [2, 3200, 1024], P(None, 'dp')
Outputs:
- output 1: bfloat16 [4, 1024, 3200], P('rep'), parts along dimension 0
- output 2: bfloat16 [4, 1024, 3200], P('rep'), parts along dimension 0
- output 3: bfloat16 [4, 3200, 1024], P('rep'), parts along dimension 0
- output 4: float32 [4, 1024, 3200], P('rep', 'dp'), parts along dimension 0
- output 5: float32 [4, 1024, 3200], P('rep', 'dp'), parts along dimension 0
- output 6: float32 [4, 3200, 1024], P('rep', 'dp'), parts along dimension 0
- output 7: float32 [4, 1024, 3200], P('rep', 'dp'), parts along dimension 0
- output 8: float32 [4, 1024, 3200], P('rep', 'dp'), parts along dimension 0
- output 9: float32 [4, 3200, 1024], P('rep', 'dp'), parts along dimension 0
There are 2 independent parts. The reference program is written for one: setup_inputs(seed, part) draws one part's arguments, and reference() takes and returns one part's arrays. A program takes and returns all parts, laid end to end along the dimension named above; an argument that names none is the same for every part.
All inputs are finite; a program needn't handle non-finite values.
Results may differ from the reference program's by a relative error of at most 0.022.
Values are sent between devices in bfloat16 or wider.
A program may use at most 768 MiB of HBM per device.

```python
import jax
import jax.numpy as jnp
from jax import lax

SEQUENCES = 16
TOKENS = 2048
D = 1024
FF = 3200
LAYERS = 2
NAMES = ("w_gate", "w_up", "w_down")
SHAPES = {"w_gate": (LAYERS, D, FF), "w_up": (LAYERS, D, FF), "w_down": (LAYERS, FF, D)}


def bump(key, n, height):
    away = (jnp.arange(n, dtype=jnp.int32) - jax.random.randint(key, (), 0, n, jnp.int32)) % n
    return jnp.where(away < n // 8, height, 1.0)


def together(key, own, strength):
    shared = jax.random.normal(key, own.shape[1:], jnp.float32)
    return (own + strength * shared) * lax.rsqrt(1 + strength * strength)


def setup_inputs(seed: int = 0, part: int = 0) -> dict:
    kx, kdy, ka, kb, kz, kf, kh, kl, *keys = jax.random.split(jax.random.key(seed), 8 + 3 * len(NAMES))
    kx, kdy, ka, kb = (jax.random.fold_in(k, part) for k in (kx, kdy, ka, kb))
    kw, km, kv = (keys[i::3] for i in range(3))
    shape = (SEQUENCES, TOKENS, D)
    much_x, much_dy = jax.random.uniform(kz, (2,), jnp.float32, 0.0, 1.0)
    loud = 2.0 ** jax.random.uniform(jax.random.fold_in(kz, 1), (), jnp.float32, -1.0, 2.0)
    layers = 2.0 ** jax.random.uniform(kl, (LAYERS, 1, 1), jnp.float32, -1.0, 1.0)
    x = together(ka, jax.random.normal(kx, shape, jnp.float32), much_x) * bump(kf, D, 4.0)
    dy = together(kb, jax.random.normal(kdy, shape, jnp.float32), much_dy)
    drawn = {"x": x.astype(jnp.bfloat16), "dy": (loud * dy * (SEQUENCES * TOKENS) ** -0.5).astype(jnp.bfloat16)}
    for key, name in zip(kw, NAMES, strict=True):
        w = jax.random.normal(key, SHAPES[name], jnp.float32) * SHAPES[name][1] ** -0.5
        drawn[name] = (w * {"w_gate": 1.0, "w_up": bump(kh, FF, 4.0), "w_down": layers}[name]).astype(jnp.bfloat16)
    for key, name in zip(km, NAMES, strict=True):
        drawn[f"m_{name}"] = 0.1 * jax.random.normal(key, SHAPES[name], jnp.float32)
    for key, name in zip(kv, NAMES, strict=True):
        drawn[f"v_{name}"] = jax.random.uniform(key, SHAPES[name], jnp.float32, 0.005, 0.015)
    return drawn


def matmul(a, w):
    return jnp.dot(a, w, preferred_element_type=jnp.float32).astype(jnp.bfloat16)


def normed(h):
    wide = h.astype(jnp.float32)
    scale = lax.rsqrt(jnp.mean(wide**2, -1, keepdims=True) + 1e-6)
    return (wide * scale).astype(jnp.bfloat16)


def layer(h, w):
    a = normed(h)
    gate = jnp.dot(a, w["w_gate"], preferred_element_type=jnp.float32)
    up = jnp.dot(a, w["w_up"], preferred_element_type=jnp.float32)
    return h + matmul((jax.nn.silu(gate) * up).astype(jnp.bfloat16), w["w_down"])


def adamw(w, m, v, g):
    m = 0.9 * m + 0.1 * g
    v = 0.95 * v + 0.05 * g * g
    step = m * lax.rsqrt(v + 1e-8) + 0.1 * w
    return (w - 0.02 * step).astype(jnp.bfloat16), m, v


def clipped(gradients, sum_of_squares, count):
    factor = jnp.minimum(1.0, 0.5 * lax.rsqrt(sum_of_squares / count + 1e-30))
    return [g * factor for g in gradients]


def stack(weights, h):
    return lax.scan(lambda h, w: (layer(h, w), None), h, weights)[0]


def reference(x, dy, w_gate, w_up, w_down, m_w_gate, m_w_up, m_w_down, v_w_gate, v_w_up, v_w_down):
    weights = dict(zip(NAMES, (w_gate, w_up, w_down), strict=True))

    def take(so_far, sequence):
        h, by_y = sequence
        _, back = jax.vjp(lambda w: stack(w, h), weights)
        return jax.tree.map(lambda total, term: total + term.astype(jnp.float32), so_far, back(by_y)[0]), None

    none_yet = {name: jnp.zeros(w.shape, jnp.float32) for name, w in weights.items()}
    by_weights, _ = lax.scan(take, none_yet, (x, dy))
    gradients = [by_weights[name].astype(jnp.bfloat16).astype(jnp.float32) for name in NAMES]
    gradients = clipped(gradients, sum(jnp.sum(g * g) for g in gradients), sum(g.size for g in gradients))
    new = [
        adamw(w.astype(jnp.float32), m, v, g)
        for w, m, v, g in zip((w_gate, w_up, w_down), (m_w_gate, m_w_up, m_w_down), (v_w_gate, v_w_up, v_w_down), gradients, strict=True)
    ]
    return tuple(one[which] for which in range(3) for one in new)
```

```python
import functools

import jax
import jax.numpy as jnp
from jax import lax
from jax.experimental import pallas as pl
from jax.experimental.pallas import tpu as pltpu
from jax.sharding import PartitionSpec as P

MESH = pl.DeviceIdType.MESH
ANY = pl.BlockSpec(memory_space=pl.ANY)
VMEM_LIMIT = 62 * 1024 * 1024
F32, BF16 = jnp.float32, jnp.bfloat16
SIDE = 4


def dot(a, b, contract):
    return lax.dot_general(a, b, (contract, ((), ())), preferred_element_type=F32)


def nn(a, b):
    return dot(a, b, ((1,), (0,)))


def nt(a, b):
    return dot(a, b, ((1,), (1,)))


def tn(a, b):
    return dot(a, b, ((0,), (0,)))


def normed(h):
    wide = h.astype(F32)
    scale = lax.rsqrt(jnp.mean(wide**2, -1, keepdims=True) + 1e-6)
    return (wide * scale).astype(BF16)


def norm_back(h, da):
    wide, da = h.astype(F32), da.astype(F32)
    scale = lax.rsqrt(jnp.mean(wide**2, -1, keepdims=True) + 1e-6)
    by_mean = jnp.sum(da * wide, -1, keepdims=True) * (-0.5 * scale * scale * scale)
    return (da * scale + wide * (by_mean * (2.0 / h.shape[-1]))).astype(BF16)


def columns(total, step):
    return [(at, min(step, total - at)) for at in range(0, total, step)]


def over_columns(total, step, body):
    whole = total // step

    def one(j, _):
        body(pl.multiple_of(j * step, step), step)
        return 0

    lax.fori_loop(0, whole, one, 0)
    if total % step:
        body(whole * step, total % step)


class Work:
    def __init__(self, grid, ins, outs, body, flops):
        self.grid, self.ins, self.outs, self.body, self.flops = grid, ins, outs, body, flops


def once(shape, index):
    return pl.BlockSpec(shape, index, pipeline_mode=pl.Buffered(1))


def gate_up(a, wg, wu, n, rows):
    t, d = a.shape
    ff = wg.shape[2]

    def body(a, wg, wu, gate, up, act):
        def piece(at, size):
            cols = pl.ds(at, size)
            g, u = nn(a[...], wg[:, cols]), nn(a[...], wu[:, cols])
            gate[:, cols] = g
            up[:, cols] = u
            act[:, cols] = (g * jax.nn.sigmoid(g) * u).astype(BF16)

        over_columns(ff, 512, piece)

    row = lambda width: pl.BlockSpec((rows, width), lambda i: (i, 0))
    weight = once((None, d, ff), lambda i: (n, 0, 0))
    return Work(
        (t // rows,),
        [(a, row(d)), (wg, weight), (wu, weight)],
        [((t, ff), F32, row(ff)), ((t, ff), F32, row(ff)), ((t, ff), BF16, row(ff))],
        body,
        4 * t * d * ff,
    )


def down(act, wd, x, n, rows):
    t, ff = act.shape
    d = wd.shape[2]

    def body(act, wd, x, h, a):
        for at, size in columns(d, 512):
            h[:, at : at + size] = x[:, at : at + size] + nn(act[...], wd[:, at : at + size]).astype(BF16)
        a[...] = normed(h[...])

    row = lambda width: pl.BlockSpec((rows, width), lambda i: (i, 0))
    return Work(
        (t // rows,),
        [(act, row(ff)), (wd, once((None, ff, d), lambda i: (n, 0, 0))), (x, row(d))],
        [((t, d), BF16, row(d)), ((t, d), BF16, row(d))],
        body,
        2 * t * d * ff,
    )


def silu_back(g, u, dact):
    s = jax.nn.sigmoid(g)
    silu = g * s
    return (dact * u * (s + silu * (1.0 - s))).astype(BF16), (dact * silu).astype(BF16)


def last_layer(a, dy, wg, wu, wd, n, rows):
    t, d = a.shape
    ff = wg.shape[2]

    def body(a, dy, wg, wu, wd, act, dgu):
        def piece(at, size):
            cols = pl.ds(at, size)
            g, u = nn(a[...], wg[:, cols]), nn(a[...], wu[:, cols])
            dact = nt(dy[...], wd[cols, :]).astype(BF16).astype(F32)
            s = jax.nn.sigmoid(g)
            silu = g * s
            act[:, cols] = (silu * u).astype(BF16)
            dgu[0, :, cols] = (dact * u * (s + silu * (1.0 - s))).astype(BF16)
            dgu[1, :, cols] = (dact * silu).astype(BF16)

        over_columns(ff, 512, piece)

    row = lambda width: pl.BlockSpec((rows, width), lambda i: (i, 0))
    weight = once((None, d, ff), lambda i: (n, 0, 0))
    return Work(
        (t // rows,),
        [(a, row(d)), (dy, row(d)), (wg, weight), (wu, weight), (wd, once((None, ff, d), lambda i: (n, 0, 0)))],
        [((t, ff), BF16, row(ff)), ((2, t, ff), BF16, pl.BlockSpec((2, rows, ff), lambda i: (0, i, 0)))],
        body,
        6 * t * d * ff,
    )


def hidden_back(dh, wd, gate, up, n, rows):
    t, d = dh.shape
    ff = wd.shape[1]

    def body(dh, wd, gate, up, dgu):
        def piece(at, size):
            cols = pl.ds(at, size)
            dact = nt(dh[...], wd[cols, :]).astype(BF16).astype(F32)
            dgu[0, :, cols], dgu[1, :, cols] = silu_back(gate[:, cols], up[:, cols], dact)

        over_columns(ff, 512, piece)

    row = lambda width: pl.BlockSpec((rows, width), lambda i: (i, 0))
    return Work(
        (t // rows,),
        [(dh, row(d)), (wd, once((None, ff, d), lambda i: (n, 0, 0))), (gate, row(ff)), (up, row(ff))],
        [((2, t, ff), BF16, pl.BlockSpec((2, rows, ff), lambda i: (0, i, 0)))],
        body,
        2 * t * d * ff,
    )


def input_back(dgu, wg, wu, h, dy, n, rows):
    _, t, ff = dgu.shape
    d = wg.shape[1]

    def body(dgu, wg, wu, h, dy, out, da):
        for at, size in columns(d, 512):
            cols = slice(at, at + size)
            da[:, cols] = nt(dgu[0], wg[cols, :]).astype(BF16) + nt(dgu[1], wu[cols, :]).astype(BF16)
        out[...] = dy[...] + norm_back(h[...], da[...])

    row = lambda width: pl.BlockSpec((rows, width), lambda i: (i, 0))
    weight = once((None, d, ff), lambda i: (n, 0, 0))
    return Work(
        (t // rows,),
        [(dgu, pl.BlockSpec((2, rows, ff), lambda i: (0, i, 0))), (wg, weight), (wu, weight), (h, row(d)), (dy, row(d))],
        [((t, d), BF16, row(d)), ((t, d), BF16, row(d))],
        body,
        4 * t * d * ff,
    )


def by_down(act, dh, tile):
    t, ff = act.shape
    d = dh.shape[1]

    def body(act, dh, out):
        out[...] = tn(act[...], dh[...]).astype(BF16)

    return Work(
        (ff // tile,),
        [(act, pl.BlockSpec((t, tile), lambda i: (0, i))), (dh, once((t, d), lambda i: (0, 0)))],
        [((ff, d), BF16, pl.BlockSpec((tile, d), lambda i: (i, 0)))],
        body,
        2 * t * d * ff,
    )


def by_gate_up(a, dgu, tile):
    t, d = a.shape
    ff = dgu.shape[2]
    tiles = ff // tile

    def body(a, dgu, out):
        out[...] = tn(a[...], dgu[...]).astype(BF16)

    return Work(
        (2 * tiles,),
        [(a, once((t, d), lambda i: (0, 0))), (dgu, pl.BlockSpec((None, t, tile), lambda i: (i // tiles, 0, i % tiles)))],
        [((2, d, ff), BF16, pl.BlockSpec((None, d, tile), lambda i: (i // tiles, 0, i % tiles)))],
        body,
        4 * t * d * ff,
    )


class Split:
    def __init__(self, rows, width, by_rows):
        self.rows, self.width, self.by_rows = rows, width, by_rows
        first = (width // 128 + 1) // 2 * 128
        self.colours = [(0, first), (first, width - first)]

    def part(self, colour, half):
        at, size = self.colours[colour]
        if self.by_rows:
            return pl.ds(half * (self.rows // 2), self.rows // 2), pl.ds(at, size)
        return pl.ds(0, self.rows), pl.ds(at + half * (size // 2), size // 2)

    def piece(self, colour):
        size = self.colours[colour][1]
        return (self.rows // 2, size) if self.by_rows else (self.rows, size // 2)

    def join(self, colours):
        along = 0 if self.by_rows else 1
        return jnp.concatenate([jnp.concatenate([c[0], c[1]], along) for c in colours], 1)


def position():
    me = lax.axis_index("dp")
    return lax.div(me, SIDE), lax.rem(me, SIDE)


def along(axis, at):
    x, y = position()
    return at * SIDE + y if axis == 0 else x * SIDE + at


def neighbours():
    x, y = position()
    for axis, here in ((0, x), (1, y)):
        for step in (1, SIDE - 1):
            yield along(axis, lax.rem(here + step, SIDE))


class Ring:
    def __init__(self, axis, source, own, scratch):
        self.axis, self.source, self.own = axis, source, own
        self.far, self.near, self.sums, self.terms, self.mine, self.send, self.recv, self.load = scratch
        here = position()[axis]
        self.here, self.right, self.left = here, lax.rem(here + 1, SIDE), lax.rem(here + SIDE - 1, SIDE)
        self.across = lax.rem(here + 2, SIDE)

    def message(self, i):
        src, dst = (
            (lambda: self.source(0, self.across), self.far.at[0]),
            (lambda: self.source(1, self.across), self.far.at[1]),
            (lambda: self.source(1, self.right), self.near.at[1]),
            (lambda: self.source(0, self.left), self.near.at[0]),
            (lambda: self.far.at[0], self.sums.at[0]),
            (lambda: self.far.at[1], self.sums.at[1]),
        )[i]
        to = self.right if i % 2 == 0 else self.left
        return pltpu.make_async_remote_copy(
            src_ref=src(),
            dst_ref=dst,
            send_sem=self.send.at[i],
            recv_sem=self.recv.at[i],
            device_id={"dp": along(self.axis, to)},
            device_id_type=MESH,
        )

    def local(self, i):
        src, dst = (
            (lambda: self.source(0, self.right), self.terms.at[0]),
            (lambda: self.source(1, self.left), self.terms.at[1]),
            (lambda: self.own(0), self.mine.at[0]),
            (lambda: self.own(1), self.mine.at[1]),
        )[i]
        return pltpu.make_async_copy(src(), dst, self.load.at[i])

    def start(self, first):
        for i in (0, 1) if first else (2, 3):
            self.message(i).start()

    def start_loads(self):
        for i in range(4):
            self.local(i).start()

    def relay(self):
        for half in (0, 1):
            self.local(half).wait()
            self.message(half).wait()
            self.far[half] = (self.far[half].astype(F32) + self.terms[half].astype(F32)).astype(BF16)
            self.message(4 + half).start()

    def finish(self, take):
        for half in (0, 1):
            self.local(2 + half).wait()
        for i in (2, 3, 4, 5):
            self.message(i).wait()
        for half in (0, 1):
            take(half)


def ring_scratch(shape, own_type):
    return [
        pltpu.VMEM((2, *shape), BF16),
        pltpu.VMEM((2, *shape), BF16),
        pltpu.VMEM((2, *shape), BF16),
        pltpu.VMEM((2, *shape), BF16),
        pltpu.VMEM((2, *shape), own_type),
        pltpu.SemaphoreType.DMA((6,)),
        pltpu.SemaphoreType.DMA((6,)),
        pltpu.SemaphoreType.DMA((4,)),
    ]


RING_SCRATCH = 8


class First:
    def __init__(self, term, split):
        self.term, self.split = term, split

    def ins(self):
        return [(self.term, ANY)]

    def outs(self):
        made = []
        for colour in (0, 1):
            piece = self.split.piece(colour)
            for shape, kind in (((2, SIDE, *piece), BF16), ((2, *piece), F32)):
                made.append((shape, kind, pl.BlockSpec(shape, lambda i, n=len(shape): (0,) * n)))
        return made

    def scratch(self):
        return [s for colour in (0, 1) for s in ring_scratch((SIDE, *self.split.piece(colour)), BF16)]

    def rings(self, ins, outs, scratch):
        (term,) = ins
        made = []
        for colour in (0, 1):

            def source(half, at, colour=colour):
                rows, cols = self.split.part(colour, half)
                return term.at[at, :, rows, cols] if colour == 0 else term.at[:, at, rows, cols]

            axis = colour
            ring = Ring(axis, source, lambda half, s=source, axis=axis: s(half, position()[axis]), scratch[colour * RING_SCRATCH :][:RING_SCRATCH])
            made.append((ring, functools.partial(self.take, ring, outs[2 * colour], outs[2 * colour + 1], 1 - axis)))
        return made

    def take(self, ring, out, own, other, half):
        total = lambda at: ring.mine[half, at].astype(F32) + ring.sums[half, at].astype(F32) + ring.near[half, at].astype(F32)
        for at in range(SIDE):
            out[half, at] = total(at).astype(BF16)
        own[half] = total(position()[other])


class Second:
    def __init__(self, parts, split):
        self.parts, self.split = parts, split

    def ins(self):
        return [(p, ANY) for p in self.parts]

    def outs(self):
        shapes = [(2, *self.split.piece(colour)) for colour in (0, 1)]
        return [(shape, BF16, pl.BlockSpec(shape, lambda i: (0, 0, 0))) for shape in shapes]

    def scratch(self):
        return [s for colour in (0, 1) for s in ring_scratch(self.split.piece(colour), F32)]

    def rings(self, ins, outs, scratch):
        made = []
        for colour in (0, 1):
            part, own = ins[2 * colour : 2 * colour + 2]
            ring = Ring(
                1 - colour,
                lambda half, at, part=part: part.at[half, at],
                lambda half, own=own: own.at[half],
                scratch[colour * RING_SCRATCH :][:RING_SCRATCH],
            )
            made.append((ring, functools.partial(self.take, ring, outs[colour])))
        return made

    def take(self, ring, out, half):
        out[half] = (ring.mine[half] + ring.sums[half].astype(F32) + ring.near[half].astype(F32)).astype(BF16)


def run(work=None, first=None, second=None, name=None, number=None, relay=(0.3, 0.5)):
    parts = [p for p in (second, first) if p is not None]
    grid = work.grid if work else (1,)
    steps = grid[0]
    groups = ([work] if work else []) + parts
    ins = [list(work.ins)] if work else []
    ins += [p.ins() for p in parts]
    outs = [list(work.outs)] if work else []
    outs += [p.outs() for p in parts]
    scratch = [p.scratch() for p in parts]

    def cut(refs, sizes):
        made = []
        for size in sizes:
            made.append(refs[:size])
            refs = refs[size:]
        return made

    n_in, n_out = sum(map(len, ins)), sum(map(len, outs))

    def kernel(*refs):
        in_refs = cut(refs[:n_in], [len(i) for i in ins])
        out_refs = cut(refs[n_in : n_in + n_out], [len(o) for o in outs])
        scratch_refs = cut(refs[n_in + n_out :], [len(s) for s in scratch])
        step = pl.program_id(0)
        skip = 1 if work else 0
        rings = [p.rings(in_refs[skip + i], out_refs[skip + i], scratch_refs[i]) for i, p in enumerate(parts)]
        if parts:

            @pl.when(step == 0)
            def _():
                barrier = pltpu.get_barrier_semaphore()
                for device in neighbours():
                    pl.semaphore_signal(barrier, inc=1, device_id={"dp": device}, device_id_type=MESH)
                pl.semaphore_wait(barrier, 4)
                for first_ones in (True, False):
                    for group in rings:
                        for ring, _ in group:
                            ring.start(first_ones)
                for group in rings:
                    for ring, _ in group:
                        ring.start_loads()

            for i, group in enumerate(rings):
                at = int(steps * (relay[i] if len(rings) == 2 else relay[1]))

                @pl.when(step == at)
                def _():
                    for ring, _ in group:
                        ring.relay()

        if work:
            work.body(*in_refs[0], *out_refs[0])
        if parts:

            @pl.when(step == steps - 1)
            def _():
                for group in rings:
                    for ring, take in group:
                        ring.finish(take)

    made = pl.pallas_call(
        kernel,
        out_shape=[jax.ShapeDtypeStruct(shape, kind) for group in outs for shape, kind, _ in group],
        grid_spec=pltpu.PrefetchScalarGridSpec(
            num_scalar_prefetch=0,
            grid=grid,
            in_specs=[spec for group in ins for _, spec in group],
            out_specs=[spec for group in outs for _, _, spec in group],
            scratch_shapes=[s for group in scratch for s in group],
        ),
        compiler_params=pltpu.CompilerParams(
            dimension_semantics=("arbitrary",),
            vmem_limit_bytes=VMEM_LIMIT,
            **(dict(collective_id=number, has_side_effects=True) if parts else {}),
        ),
        cost_estimate=pl.CostEstimate(flops=work.flops if work else 1000, bytes_accessed=1 << 24, transcendentals=0),
        name=name,
    )(*[a for group in ins for a, _ in group])
    return cut(made, [len(o) for o in outs])


def everywhere(own, number, members):
    def kernel(own, out, send, recv, load):
        me = lax.axis_index("dp")
        barrier = pltpu.get_barrier_semaphore()
        peers = [lax.rem(me + i, members) for i in range(1, members)]
        for peer in peers:
            pl.semaphore_signal(barrier, inc=1, device_id={"dp": peer}, device_id_type=MESH)
        pl.semaphore_wait(barrier, members - 1)
        keep = pltpu.make_async_copy(own, out.at[me], load)
        keep.start()

        def copy(i, slot):
            return pltpu.make_async_remote_copy(
                src_ref=own, dst_ref=out.at[slot], send_sem=send.at[i], recv_sem=recv.at[i], device_id={"dp": peers[i]}, device_id_type=MESH
            )

        for i in range(members - 1):
            copy(i, me).start()
        keep.wait()
        for i in range(members - 1):
            copy(i, me).wait_send()
            copy(i, lax.rem(me + members - 1 - i, members)).wait_recv()

    return pl.pallas_call(
        kernel,
        out_shape=jax.ShapeDtypeStruct((members, *own.shape), own.dtype),
        in_specs=[ANY],
        out_specs=pl.BlockSpec(memory_space=pl.ANY),
        scratch_shapes=[pltpu.SemaphoreType.DMA((members - 1,)), pltpu.SemaphoreType.DMA((members - 1,)), pltpu.SemaphoreType.DMA],
        compiler_params=pltpu.CompilerParams(collective_id=number, has_side_effects=True),
        name="everywhere",
    )(own)


def adamw(w, m, v, g):
    m = 0.9 * m + 0.1 * g
    v = 0.95 * v + 0.05 * g * g
    step = m * lax.rsqrt(v + 1e-8) + 0.1 * w
    return (w - 0.02 * step).astype(BF16), m, v


def solution(mesh):
    members = mesh.shape["dp"]

    def step(x, dy, wg, wu, wd, *moments):
        x, dy = x[0], dy[0]
        d, ff = wg.shape[1:]
        wide, tall = Split(d // members, ff, True), Split(ff // members, d, False)
        square = lambda t: t.reshape(SIDE, SIDE, t.shape[0] // members, t.shape[1])

        a0 = normed(x)
        [[gate0, up0, act0]] = run(gate_up(a0, wg, wu, 0, 256), name="gate_up_0")
        [[h1, a1]] = run(down(act0, wd, x, 0, 512), name="down_0")
        [[act1, dgu1]] = run(last_layer(a1, dy, wg, wu, wd, 1, 256), name="layer_1")
        [[d1]] = run(by_down(act1, dy, 640), name="by_down_1")
        [[gu1], d1_half] = run(by_gate_up(a1, dgu1, 640), First(square(d1), tall), name="by_gate_up_1", number=1)
        [[dh1, _], d1_sum, g1_half] = run(
            input_back(dgu1, wg, wu, h1, dy, 1, 256), First(square(gu1[0]), wide), Second(d1_half, tall), name="input_back_1", number=2
        )
        [[dgu0], g1_sum, u1_half] = run(
            hidden_back(dh1, wd, gate0, up0, 0, 256), First(square(gu1[1]), wide), Second(g1_half, wide), name="hidden_back_0", number=3
        )
        [[d0], u1_sum] = run(by_down(act0, dh1, 640), None, Second(u1_half, wide), name="by_down_0", number=4)
        [[gu0], d0_half] = run(by_gate_up(a0, dgu0, 640), First(square(d0), tall), name="by_gate_up_0", number=5)
        d0_sum, g0_half = run(None, First(square(gu0[0]), wide), Second(d0_half, tall), name="sum_gate_0", number=6)
        g0_sum, u0_half = run(None, First(square(gu0[1]), wide), Second(g0_half, wide), name="sum_up_0", number=7)
        [u0_sum] = run(None, None, Second(u0_half, wide), name="sum_end", number=8)

        g = [
            jnp.stack([split.join(one) for one in sums]).astype(F32)
            for split, sums in ((wide, (g0_sum, g1_sum)), (wide, (u0_sum, u1_sum)), (tall, (d0_sum, d1_sum)))
        ]
        squares = jnp.broadcast_to(sum(jnp.sum(one * one) for one in g), (8, 128))
        squares = jnp.sum(everywhere(squares, 9, members)[:, 0, 0])
        count = sum(w.size for w in (wg, wu, wd))
        factor = jnp.minimum(1.0, 0.5 * lax.rsqrt(squares / count + 1e-30))
        me = lax.axis_index("dp")
        new = []
        for w, m, v, one in zip((wg, wu, wd), moments[:3], moments[3:], g, strict=True):
            rows = w.shape[1] // members
            mine = lax.dynamic_slice_in_dim(w, me * rows, rows, 1).astype(F32)
            w, m, v = adamw(mine, m, v, one * factor)
            new.append((lax.all_gather(w, "dp", axis=1, tiled=True), m, v))
        return tuple(one[which] for which in range(3) for one in new)

    parts, whole, moment, out = P(("rep", "dp"), None, None), P(None, None, None), P(None, "dp", None), P("rep", "dp", None)
    return jax.shard_map(
        step,
        mesh=mesh,
        in_specs=(parts,) * 2 + (whole,) * 3 + (moment,) * 6,
        out_specs=(P("rep", None, None),) * 3 + (out,) * 6,
        check_vma=False,
    )
```

```python
import functools

import jax
import jax.numpy as jnp
from jax import lax
from jax.experimental import pallas as pl
from jax.experimental.pallas import tpu as pltpu
from jax.sharding import PartitionSpec as P

MESH = pl.DeviceIdType.MESH
ANY = pl.BlockSpec(memory_space=pl.ANY)
VMEM_LIMIT = 62 * 1024 * 1024
F32, BF16 = jnp.float32, jnp.bfloat16
SIDE = 4


def dot(a, b, contract):
    return lax.dot_general(a, b, (contract, ((), ())), preferred_element_type=F32)


def nn(a, b):
    return dot(a, b, ((1,), (0,)))


def nt(a, b):
    return dot(a, b, ((1,), (1,)))


def tn(a, b):
    return dot(a, b, ((0,), (0,)))


def normed(h):
    wide = h.astype(F32)
    scale = lax.rsqrt(jnp.mean(wide**2, -1, keepdims=True) + 1e-6)
    return (wide * scale).astype(BF16)


def norm_back(h, da):
    wide, da = h.astype(F32), da.astype(F32)
    scale = lax.rsqrt(jnp.mean(wide**2, -1, keepdims=True) + 1e-6)
    by_mean = jnp.sum(da * wide, -1, keepdims=True) * (-0.5 * scale * scale * scale)
    return (da * scale + wide * (by_mean * (2.0 / h.shape[-1]))).astype(BF16)


def sigmoid(g):
    return 0.5 * jnp.tanh(0.5 * g) + 0.5


def columns(total, step):
    return [(at, min(step, total - at)) for at in range(0, total, step)]


class Work:
    def __init__(self, grid, ins, outs, body, flops):
        self.grid, self.ins, self.outs, self.body, self.flops = grid, ins, outs, body, flops


def once(shape, index):
    return pl.BlockSpec(shape, index, pipeline_mode=pl.Buffered(1))


def gate_up(a, wg, wu, n, rows):
    t, d = a.shape
    ff = wg.shape[2]

    def body(a, wg, wu, gate, up, act):
        for at, size in columns(ff, 512):
            cols = pl.ds(at, size)
            g, u = nn(a[...], wg[:, cols]), nn(a[...], wu[:, cols])
            gate[:, cols] = g
            up[:, cols] = u
            act[:, cols] = (g * sigmoid(g) * u).astype(BF16)

    row = lambda width: pl.BlockSpec((rows, width), lambda i: (i, 0))
    weight = once((None, d, ff), lambda i: (n, 0, 0))
    return Work(
        (t // rows,),
        [(a, row(d)), (wg, weight), (wu, weight)],
        [((t, ff), F32, row(ff)), ((t, ff), F32, row(ff)), ((t, ff), BF16, row(ff))],
        body,
        4 * t * d * ff,
    )


def down(act, wd, x, n, rows):
    t, ff = act.shape
    d = wd.shape[2]

    def body(act, wd, x, h, a):
        for at, size in columns(d, 512):
            h[:, at : at + size] = x[:, at : at + size] + nn(act[...], wd[:, at : at + size]).astype(BF16)
        a[...] = normed(h[...])

    row = lambda width: pl.BlockSpec((rows, width), lambda i: (i, 0))
    return Work(
        (t // rows,),
        [(act, row(ff)), (wd, once((None, ff, d), lambda i: (n, 0, 0))), (x, row(d))],
        [((t, d), BF16, row(d)), ((t, d), BF16, row(d))],
        body,
        2 * t * d * ff,
    )


def silu_back(g, u, dact):
    s = sigmoid(g)
    silu = g * s
    return (dact * u * (s + silu * (1.0 - s))).astype(BF16), (dact * silu).astype(BF16)


def last_layer(a, dy, wg, wu, wd, n, rows):
    t, d = a.shape
    ff = wg.shape[2]

    def body(a, dy, wg, wu, wd, act, dgu):
        for at, size in columns(ff, 512):
            cols = pl.ds(at, size)
            g, u = nn(a[...], wg[:, cols]), nn(a[...], wu[:, cols])
            dact = nt(dy[...], wd[cols, :]).astype(BF16).astype(F32)
            act[:, cols] = (g * sigmoid(g) * u).astype(BF16)
            dgu[0, :, cols], dgu[1, :, cols] = silu_back(g, u, dact)

    row = lambda width: pl.BlockSpec((rows, width), lambda i: (i, 0))
    weight = once((None, d, ff), lambda i: (n, 0, 0))
    return Work(
        (t // rows,),
        [(a, row(d)), (dy, row(d)), (wg, weight), (wu, weight), (wd, once((None, ff, d), lambda i: (n, 0, 0)))],
        [((t, ff), BF16, row(ff)), ((2, t, ff), BF16, pl.BlockSpec((2, rows, ff), lambda i: (0, i, 0)))],
        body,
        6 * t * d * ff,
    )


def hidden_back(dh, wd, gate, up, n, rows):
    t, d = dh.shape
    ff = wd.shape[1]

    def body(dh, wd, gate, up, dgu):
        for at, size in columns(ff, 512):
            cols = pl.ds(at, size)
            dact = nt(dh[...], wd[cols, :]).astype(BF16).astype(F32)
            dgu[0, :, cols], dgu[1, :, cols] = silu_back(gate[:, cols], up[:, cols], dact)

    row = lambda width: pl.BlockSpec((rows, width), lambda i: (i, 0))
    return Work(
        (t // rows,),
        [(dh, row(d)), (wd, once((None, ff, d), lambda i: (n, 0, 0))), (gate, row(ff)), (up, row(ff))],
        [((2, t, ff), BF16, pl.BlockSpec((2, rows, ff), lambda i: (0, i, 0)))],
        body,
        2 * t * d * ff,
    )


def input_back(dgu, wg, wu, h, dy, n, rows):
    _, t, ff = dgu.shape
    d = wg.shape[1]

    def body(dgu, wg, wu, h, dy, out, da):
        for at, size in columns(d, 512):
            cols = slice(at, at + size)
            da[:, cols] = nt(dgu[0], wg[cols, :]).astype(BF16) + nt(dgu[1], wu[cols, :]).astype(BF16)
        out[...] = dy[...] + norm_back(h[...], da[...])

    row = lambda width: pl.BlockSpec((rows, width), lambda i: (i, 0))
    weight = once((None, d, ff), lambda i: (n, 0, 0))
    return Work(
        (t // rows,),
        [(dgu, pl.BlockSpec((2, rows, ff), lambda i: (0, i, 0))), (wg, weight), (wu, weight), (h, row(d)), (dy, row(d))],
        [((t, d), BF16, row(d)), ((t, d), BF16, row(d))],
        body,
        4 * t * d * ff,
    )


def by_down(act, dh, tile):
    t, ff = act.shape
    d = dh.shape[1]

    def body(act, dh, out):
        out[...] = tn(act[...], dh[...]).astype(BF16)

    return Work(
        (ff // tile,),
        [(act, pl.BlockSpec((t, tile), lambda i: (0, i))), (dh, once((t, d), lambda i: (0, 0)))],
        [((1, ff, d), BF16, pl.BlockSpec((None, tile, d), lambda i: (0, i, 0)))],
        body,
        2 * t * d * ff,
    )


def by_gate_up(a, dgu, tile, which):
    t, d = a.shape
    ff = dgu.shape[2]
    tiles, low = ff // tile, min(which)

    def body(a, dgu, out):
        out[...] = tn(dgu[...], a[...]).astype(BF16).T

    return Work(
        (len(which) * tiles,),
        [(a, once((t, d), lambda i: (0, 0))), (dgu, pl.BlockSpec((None, t, tile), lambda i: (low + i // tiles, 0, i % tiles)))],
        [((len(which), d, ff), BF16, pl.BlockSpec((None, d, tile), lambda i: (i // tiles, 0, i % tiles)))],
        body,
        2 * len(which) * t * d * ff,
    )


class Split:
    def __init__(self, rows, width, by_rows):
        self.rows, self.width, self.by_rows = rows, width, by_rows
        first = (width // 128 + 1) // 2 * 128
        self.colours = [(0, first), (first, width - first)]

    def part(self, colour, half):
        at, size = self.colours[colour]
        if self.by_rows:
            return pl.ds(half * (self.rows // 2), self.rows // 2), pl.ds(at, size)
        return pl.ds(0, self.rows), pl.ds(at + half * (size // 2), size // 2)

    def piece(self, colour):
        size = self.colours[colour][1]
        return (self.rows // 2, size) if self.by_rows else (self.rows, size // 2)

    def join(self, colours):
        along = 0 if self.by_rows else 1
        return jnp.concatenate([jnp.concatenate([c[0], c[1]], along) for c in colours], 1)


def position():
    me = lax.axis_index("dp")
    return lax.div(me, SIDE), lax.rem(me, SIDE)


def along(axis, at):
    x, y = position()
    return at * SIDE + y if axis == 0 else x * SIDE + at


def neighbours():
    x, y = position()
    for axis, here in ((0, x), (1, y)):
        for step in (1, SIDE - 1):
            yield along(axis, lax.rem(here + step, SIDE))


class Ring:
    def __init__(self, axis, source, own, scratch):
        self.axis, self.source, self.own = axis, source, own
        self.far, self.near, self.sums, self.terms, self.mine, self.send, self.recv, self.load = scratch
        here = position()[axis]
        self.here, self.right, self.left = here, lax.rem(here + 1, SIDE), lax.rem(here + SIDE - 1, SIDE)
        self.across = lax.rem(here + 2, SIDE)

    def message(self, i):
        src, dst = (
            (lambda: self.source(0, self.across), self.far.at[0]),
            (lambda: self.source(1, self.across), self.far.at[1]),
            (lambda: self.source(1, self.right), self.near.at[1]),
            (lambda: self.source(0, self.left), self.near.at[0]),
            (lambda: self.far.at[0], self.sums.at[0]),
            (lambda: self.far.at[1], self.sums.at[1]),
        )[i]
        to = self.right if i % 2 == 0 else self.left
        return pltpu.make_async_remote_copy(
            src_ref=src(),
            dst_ref=dst,
            send_sem=self.send.at[i],
            recv_sem=self.recv.at[i],
            device_id={"dp": along(self.axis, to)},
            device_id_type=MESH,
        )

    def local(self, i):
        src, dst = (
            (lambda: self.source(0, self.right), self.terms.at[0]),
            (lambda: self.source(1, self.left), self.terms.at[1]),
            (lambda: self.own(0), self.mine.at[0]),
            (lambda: self.own(1), self.mine.at[1]),
        )[i]
        return pltpu.make_async_copy(src(), dst, self.load.at[i])

    def start(self, first):
        for i in (0, 1) if first else (2, 3):
            self.message(i).start()

    def start_loads(self):
        for i in range(4):
            self.local(i).start()

    def relay(self):
        for half in (0, 1):
            self.local(half).wait()
            self.message(half).wait()
            self.far[half] = (self.far[half].astype(F32) + self.terms[half].astype(F32)).astype(BF16)
            self.message(4 + half).start()

    def finish(self, take):
        for half in (0, 1):
            self.local(2 + half).wait()
        for i in (2, 3, 4, 5):
            self.message(i).wait()
        for half in (0, 1):
            take(half)


def ring_scratch(shape, own_type):
    return [
        pltpu.VMEM((2, *shape), BF16),
        pltpu.VMEM((2, *shape), BF16),
        pltpu.VMEM((2, *shape), BF16),
        pltpu.VMEM((2, *shape), BF16),
        pltpu.VMEM((2, *shape), own_type),
        pltpu.SemaphoreType.DMA((6,)),
        pltpu.SemaphoreType.DMA((6,)),
        pltpu.SemaphoreType.DMA((4,)),
    ]


RING_SCRATCH = 8


class First:
    def __init__(self, terms, which, split):
        self.term, self.which, self.split = terms, which, split

    def ins(self):
        return [(self.term, ANY)]

    def outs(self):
        made = []
        for colour in (0, 1):
            piece = self.split.piece(colour)
            for shape, kind in (((2, SIDE, *piece), BF16), ((2, *piece), F32)):
                made.append((shape, kind, pl.BlockSpec(shape, lambda i, n=len(shape): (0,) * n)))
        return made

    def scratch(self):
        return [s for colour in (0, 1) for s in ring_scratch((SIDE, *self.split.piece(colour)), BF16)]

    def rings(self, ins, outs, scratch):
        (term,) = ins
        made = []
        for colour in (0, 1):

            def source(half, at, colour=colour):
                rows, cols = self.split.part(colour, half)
                return term.at[self.which, at, :, rows, cols] if colour == 0 else term.at[self.which, :, at, rows, cols]

            axis = colour
            ring = Ring(axis, source, lambda half, s=source, axis=axis: s(half, position()[axis]), scratch[colour * RING_SCRATCH :][:RING_SCRATCH])
            made.append((ring, functools.partial(self.take, ring, outs[2 * colour], outs[2 * colour + 1], 1 - axis)))
        return made

    def take(self, ring, out, own, other, half):
        total = lambda at: ring.mine[half, at].astype(F32) + ring.sums[half, at].astype(F32) + ring.near[half, at].astype(F32)
        for at in range(SIDE):
            out[half, at] = total(at).astype(BF16)
        own[half] = total(position()[other])


class Second:
    def __init__(self, parts, split):
        self.parts, self.split = parts, split

    def ins(self):
        return [(p, ANY) for p in self.parts]

    def outs(self):
        shapes = [(2, *self.split.piece(colour)) for colour in (0, 1)]
        return [(shape, BF16, pl.BlockSpec(shape, lambda i: (0, 0, 0))) for shape in shapes]

    def scratch(self):
        return [s for colour in (0, 1) for s in ring_scratch(self.split.piece(colour), F32)]

    def rings(self, ins, outs, scratch):
        made = []
        for colour in (0, 1):
            part, own = ins[2 * colour : 2 * colour + 2]
            ring = Ring(
                1 - colour,
                lambda half, at, part=part: part.at[half, at],
                lambda half, own=own: own.at[half],
                scratch[colour * RING_SCRATCH :][:RING_SCRATCH],
            )
            made.append((ring, functools.partial(self.take, ring, outs[colour])))
        return made

    def take(self, ring, out, half):
        out[half] = (ring.mine[half] + ring.sums[half].astype(F32) + ring.near[half].astype(F32)).astype(BF16)


def run(work=None, first=None, second=None, name=None, number=None, relay=(0.3, 0.5)):
    parts = [p for p in (second, first) if p is not None]
    grid = work.grid if work else (1,)
    steps = grid[0]
    groups = ([work] if work else []) + parts
    ins = [list(work.ins)] if work else []
    ins += [p.ins() for p in parts]
    outs = [list(work.outs)] if work else []
    outs += [p.outs() for p in parts]
    scratch = [p.scratch() for p in parts]

    def cut(refs, sizes):
        made = []
        for size in sizes:
            made.append(refs[:size])
            refs = refs[size:]
        return made

    n_in, n_out = sum(map(len, ins)), sum(map(len, outs))

    def kernel(*refs):
        in_refs = cut(refs[:n_in], [len(i) for i in ins])
        out_refs = cut(refs[n_in : n_in + n_out], [len(o) for o in outs])
        scratch_refs = cut(refs[n_in + n_out :], [len(s) for s in scratch])
        step = pl.program_id(0)
        skip = 1 if work else 0
        rings = [p.rings(in_refs[skip + i], out_refs[skip + i], scratch_refs[i]) for i, p in enumerate(parts)]
        if parts:

            @pl.when(step == 0)
            def _():
                barrier = pltpu.get_barrier_semaphore()
                for device in neighbours():
                    pl.semaphore_signal(barrier, inc=1, device_id={"dp": device}, device_id_type=MESH)
                pl.semaphore_wait(barrier, 4)
                for first_ones in (True, False):
                    for group in rings:
                        for ring, _ in group:
                            ring.start(first_ones)
                for group in rings:
                    for ring, _ in group:
                        ring.start_loads()

            for i, group in enumerate(rings):
                at = int(steps * (relay[i] if len(rings) == 2 else relay[1]))

                @pl.when(step == at)
                def _():
                    for ring, _ in group:
                        ring.relay()

        if work:
            work.body(*in_refs[0], *out_refs[0])
        if parts:

            @pl.when(step == steps - 1)
            def _():
                for group in rings:
                    for ring, take in group:
                        ring.finish(take)

    made = pl.pallas_call(
        kernel,
        out_shape=[jax.ShapeDtypeStruct(shape, kind) for group in outs for shape, kind, _ in group],
        grid_spec=pltpu.PrefetchScalarGridSpec(
            num_scalar_prefetch=0,
            grid=grid,
            in_specs=[spec for group in ins for _, spec in group],
            out_specs=[spec for group in outs for _, _, spec in group],
            scratch_shapes=[s for group in scratch for s in group],
        ),
        compiler_params=pltpu.CompilerParams(
            dimension_semantics=("arbitrary",),
            vmem_limit_bytes=VMEM_LIMIT,
            **(dict(collective_id=number, has_side_effects=True) if parts else {}),
        ),
        cost_estimate=pl.CostEstimate(flops=work.flops if work else 1000, bytes_accessed=1 << 24, transcendentals=0),
        name=name,
    )(*[a for group in ins for a, _ in group])
    return cut(made, [len(o) for o in outs])


def everywhere(own, number, members):
    def kernel(own, out, send, recv, load):
        me = lax.axis_index("dp")
        barrier = pltpu.get_barrier_semaphore()
        peers = [lax.rem(me + i, members) for i in range(1, members)]
        for peer in peers:
            pl.semaphore_signal(barrier, inc=1, device_id={"dp": peer}, device_id_type=MESH)
        pl.semaphore_wait(barrier, members - 1)
        keep = pltpu.make_async_copy(own, out.at[me], load)
        keep.start()

        def copy(i, slot):
            return pltpu.make_async_remote_copy(
                src_ref=own, dst_ref=out.at[slot], send_sem=send.at[i], recv_sem=recv.at[i], device_id={"dp": peers[i]}, device_id_type=MESH
            )

        for i in range(members - 1):
            copy(i, me).start()
        keep.wait()
        for i in range(members - 1):
            copy(i, me).wait_send()
            copy(i, lax.rem(me + members - 1 - i, members)).wait_recv()

    return pl.pallas_call(
        kernel,
        out_shape=jax.ShapeDtypeStruct((members, *own.shape), own.dtype),
        in_specs=[ANY],
        out_specs=pl.BlockSpec(memory_space=pl.ANY),
        scratch_shapes=[pltpu.SemaphoreType.DMA((members - 1,)), pltpu.SemaphoreType.DMA((members - 1,)), pltpu.SemaphoreType.DMA],
        compiler_params=pltpu.CompilerParams(collective_id=number, has_side_effects=True),
        name="everywhere",
    )(own)


class Spread:
    def __init__(self, block, out, split, colour, send, recv):
        self.block, self.out, self.split, self.colour, self.send, self.recv = block, out, split, colour, send, recv

    def region(self, stage, half, place):
        rows, cols = self.split.part(self.colour, half)
        x, y = position()
        if stage == 0:
            x, y = (place, y) if self.colour == 0 else (x, place)
            return self.out.at[:, x, y, rows, cols]
        return self.out.at[:, :, place, rows, cols] if self.colour == 0 else self.out.at[:, place, :, rows, cols]

    def message(self, stage, i, arriving=False):
        axis = self.colour if stage == 0 else 1 - self.colour
        here = position()[axis]
        right, left = lax.rem(here + 1, SIDE), lax.rem(here + SIDE - 1, SIDE)
        sender = here if not arriving else (left if i % 2 == 0 else right)
        half = (0, 1, 1, 0, 0, 1)[i]
        owner = sender if i < 4 else lax.rem(sender + (SIDE - 1 if i == 4 else 1), SIDE)
        region = self.region(stage, half, owner)
        src = region
        if stage == 0 and i < 4:
            rows, cols = self.split.part(self.colour, half)
            src = self.block.at[:, rows, cols]
        return pltpu.make_async_remote_copy(
            src_ref=src,
            dst_ref=region,
            send_sem=self.send.at[stage, i],
            recv_sem=self.recv.at[stage, i],
            device_id={"dp": along(axis, right if i % 2 == 0 else left)},
            device_id_type=MESH,
        )

    def start(self, stage, first):
        for i in (0, 1) if first else (2, 3):
            self.message(stage, i).start()

    def hand_on(self, stage):
        for i in (0, 1):
            self.message(stage, i, True).wait_recv()
            self.message(stage, 4 + i).start()

    def arrived(self, stage):
        for i in (2, 3, 4, 5):
            self.message(stage, i, True).wait_recv()

    def sent(self):
        for stage in (0, 1):
            for i in range(6):
                self.message(stage, i).wait_send()


def gathered(blocks, splits, number):
    n = len(blocks)

    def kernel(*refs):
        ins, outs, held = refs[:n], refs[n : 2 * n], refs[2 * n : 3 * n]
        send, recv, load, store = refs[3 * n :]
        spreads = [[Spread(ins[k], outs[k], splits[k], c, send.at[k, c], recv.at[k, c]) for c in (0, 1)] for k in range(n)]
        x, y = position()
        loads = [lambda k=k: pltpu.make_async_copy(ins[k], held[k], load.at[k]) for k in range(n)]
        stores = [lambda k=k: pltpu.make_async_copy(held[k], outs[k].at[:, x, y], store.at[k]) for k in range(n)]
        for k in range(n):
            loads[k]().start()
        barrier = pltpu.get_barrier_semaphore()
        for device in neighbours():
            pl.semaphore_signal(barrier, inc=1, device_id={"dp": device}, device_id_type=MESH)
        pl.semaphore_wait(barrier, 4)
        for k in range(n):
            for first in (True, False):
                for spread in spreads[k]:
                    spread.start(0, first)
        for k in range(n):
            loads[k]().wait()
            stores[k]().start()
        for k in range(n):
            for spread in spreads[k]:
                spread.hand_on(0)
        for k in range(n):
            stores[k]().wait()
            for spread in spreads[k]:
                spread.arrived(0)
            for first in (True, False):
                for spread in spreads[k]:
                    spread.start(1, first)
        for k in range(n):
            for spread in spreads[k]:
                spread.hand_on(1)
        for k in range(n):
            for spread in spreads[k]:
                spread.arrived(1)
                spread.sent()

    return pl.pallas_call(
        kernel,
        out_shape=[jax.ShapeDtypeStruct((b.shape[0], SIDE, SIDE, *b.shape[1:]), b.dtype) for b in blocks],
        in_specs=[ANY] * n,
        out_specs=[ANY] * n,
        scratch_shapes=[pltpu.VMEM(b.shape, b.dtype) for b in blocks]
        + [pltpu.SemaphoreType.DMA((n, 2, 2, 6)), pltpu.SemaphoreType.DMA((n, 2, 2, 6)), pltpu.SemaphoreType.DMA((n,)), pltpu.SemaphoreType.DMA((n,))],
        compiler_params=pltpu.CompilerParams(collective_id=number, has_side_effects=True, vmem_limit_bytes=VMEM_LIMIT),
        name="gathered",
    )(*blocks)


def adamw(w, m, v, g):
    m = 0.9 * m + 0.1 * g
    v = 0.95 * v + 0.05 * g * g
    step = m * lax.rsqrt(v + 1e-8) + 0.1 * w
    return (w - 0.02 * step).astype(BF16), m, v


def solution(mesh):
    members = mesh.shape["dp"]

    def step(x, dy, wg, wu, wd, *moments):
        x, dy = x[0], dy[0]
        d, ff = wg.shape[1:]
        wide, tall = Split(d // members, ff, True), Split(ff // members, d, False)
        square = lambda t: t.reshape(t.shape[0], SIDE, SIDE, t.shape[1] // members, t.shape[2])

        a0 = normed(x)
        [[gate0, up0, act0]] = run(gate_up(a0, wg, wu, 0, 256), name="gate_up_0")
        [[h1, a1]] = run(down(act0, wd, x, 0, 256), name="down_0")
        [[act1, dgu1]] = run(last_layer(a1, dy, wg, wu, wd, 1, 256), name="layer_1")
        [[d1]] = run(by_down(act1, dy, 640), name="by_down_1")
        [[gu1], d1_half] = run(by_gate_up(a1, dgu1, 640, (0, 1)), First(square(d1), 0, tall), name="by_gate_up_1", number=1)
        gu1 = square(gu1)
        [[dh1, _], d1_sum, g1_half] = run(
            input_back(dgu1, wg, wu, h1, dy, 1, 256), First(gu1, 0, wide), Second(d1_half, tall), name="input_back_1", number=2
        )
        [[dgu0], g1_sum, u1_half] = run(
            hidden_back(dh1, wd, gate0, up0, 0, 256), First(gu1, 1, wide), Second(g1_half, wide), name="hidden_back_0", number=3
        )
        [[d0], u1_sum] = run(by_down(act0, dh1, 640), None, Second(u1_half, wide), name="by_down_0", number=4)
        [[g0], d0_half] = run(by_gate_up(a0, dgu0, 640, (0,)), First(square(d0), 0, tall), name="by_gate_0", number=5)
        [[u0], d0_sum, g0_half] = run(by_gate_up(a0, dgu0, 640, (1,)), First(square(g0), 0, wide), Second(d0_half, tall), name="by_up_0", number=6)
        g0_sum, u0_half = run(None, First(square(u0), 0, wide), Second(g0_half, wide), name="sum_up_0", number=7)
        [u0_sum] = run(None, None, Second(u0_half, wide), name="sum_end", number=8)

        g = [
            jnp.stack([split.join(one) for one in sums]).astype(F32)
            for split, sums in ((wide, (g0_sum, g1_sum)), (wide, (u0_sum, u1_sum)), (tall, (d0_sum, d1_sum)))
        ]
        squares = jnp.broadcast_to(sum(jnp.sum(one * one) for one in g), (8, 128))
        squares = jnp.sum(everywhere(squares, 9, members)[:, 0, 0])
        count = sum(w.size for w in (wg, wu, wd))
        factor = jnp.minimum(1.0, 0.5 * lax.rsqrt(squares / count + 1e-30))
        me = lax.axis_index("dp")
        new = []
        for w, m, v, one in zip((wg, wu, wd), moments[:3], moments[3:], g, strict=True):
            rows = w.shape[1] // members
            mine = lax.dynamic_slice_in_dim(w, me * rows, rows, 1).astype(F32)
            new.append(adamw(mine, m, v, one * factor))
        weights = gathered([w for w, _, _ in new], (wide, wide, tall), 10)
        weights = [one.reshape(w.shape) for one, w in zip(weights, (wg, wu, wd), strict=True)]
        return (*weights, *(m for _, m, _ in new), *(v for _, _, v in new))

    parts, whole, moment, out = P(("rep", "dp"), None, None), P(None, None, None), P(None, "dp", None), P("rep", "dp", None)
    return jax.shard_map(
        step,
        mesh=mesh,
        in_specs=(parts,) * 2 + (whole,) * 3 + (moment,) * 6,
        out_specs=(P("rep", None, None),) * 3 + (out,) * 6,
        check_vma=False,
    )
```

```python
import functools

import jax
import jax.numpy as jnp
from jax import lax
from jax.experimental import pallas as pl
from jax.experimental.pallas import tpu as pltpu
from jax.sharding import PartitionSpec as P

MESH = pl.DeviceIdType.MESH
ANY = pl.BlockSpec(memory_space=pl.ANY)
TILE = pl.BlockSpec((8, 128), lambda i: (0, 0))
VMEM_LIMIT = 62 * 1024 * 1024
F32, BF16 = jnp.float32, jnp.bfloat16
SIDE = 4


def dot(a, b, contract):
    return lax.dot_general(a, b, (contract, ((), ())), preferred_element_type=F32)


def nn(a, b):
    return dot(a, b, ((1,), (0,)))


def nt(a, b):
    return dot(a, b, ((1,), (1,)))


def tn(a, b):
    return dot(a, b, ((0,), (0,)))


def normed(h):
    wide = h.astype(F32)
    scale = lax.rsqrt(jnp.mean(wide**2, -1, keepdims=True) + 1e-6)
    return (wide * scale).astype(BF16)


def norm_back(h, da):
    wide, da = h.astype(F32), da.astype(F32)
    scale = lax.rsqrt(jnp.mean(wide**2, -1, keepdims=True) + 1e-6)
    by_mean = jnp.sum(da * wide, -1, keepdims=True) * (-0.5 * scale * scale * scale)
    return (da * scale + wide * (by_mean * (2.0 / h.shape[-1]))).astype(BF16)


def sigmoid(g):
    return 0.5 * jnp.tanh(0.5 * g) + 0.5


def columns(total, step):
    return [(at, min(step, total - at)) for at in range(0, total, step)]


def over_columns(total, step, body):
    whole = total // step

    def one(j, _):
        body(pl.multiple_of(j * step, step), step)
        return 0

    lax.fori_loop(0, whole, one, 0)
    if total % step:
        body(whole * step, total % step)


class Work:
    def __init__(self, grid, ins, outs, body, flops):
        self.grid, self.ins, self.outs, self.body, self.flops = grid, ins, outs, body, flops


def once(shape, index):
    return pl.BlockSpec(shape, index, pipeline_mode=pl.Buffered(1))


def gate_up(x, wg, wu, n, rows):
    t, d = x.shape
    ff = wg.shape[2]

    def body(x, wg, wu, gate, up, act, a):
        a[...] = normed(x[...])
        for at, size in columns(ff, 512):
            cols = pl.ds(at, size)
            g, u = nn(a[...], wg[:, cols]), nn(a[...], wu[:, cols])
            gate[:, cols] = g
            up[:, cols] = u
            act[:, cols] = (g * sigmoid(g) * u).astype(BF16)

    row = lambda width: pl.BlockSpec((rows, width), lambda i: (i, 0))
    weight = once((None, d, ff), lambda i: (n, 0, 0))
    return Work(
        (t // rows,),
        [(x, row(d)), (wg, weight), (wu, weight)],
        [((t, ff), F32, row(ff)), ((t, ff), F32, row(ff)), ((t, ff), BF16, row(ff)), ((t, d), BF16, row(d))],
        body,
        4 * t * d * ff,
    )


def down(act, wd, x, n, rows):
    t, ff = act.shape
    d = wd.shape[2]

    def body(act, wd, x, h, a):
        for at, size in columns(d, 512):
            h[:, at : at + size] = x[:, at : at + size] + nn(act[...], wd[:, at : at + size]).astype(BF16)
        a[...] = normed(h[...])

    row = lambda width: pl.BlockSpec((rows, width), lambda i: (i, 0))
    return Work(
        (t // rows,),
        [(act, row(ff)), (wd, once((None, ff, d), lambda i: (n, 0, 0))), (x, row(d))],
        [((t, d), BF16, row(d)), ((t, d), BF16, row(d))],
        body,
        2 * t * d * ff,
    )


def silu_back(g, u, dact):
    s = sigmoid(g)
    silu = g * s
    return (dact * u * (s + silu * (1.0 - s))).astype(BF16), (dact * silu).astype(BF16)


def last_layer(a, dy, wg, wu, wd, n, rows):
    t, d = a.shape
    ff = wg.shape[2]

    def body(a, dy, wg, wu, wd, act, dgu):
        for at, size in columns(ff, 512):
            cols = pl.ds(at, size)
            g, u = nn(a[...], wg[:, cols]), nn(a[...], wu[:, cols])
            dact = nt(dy[...], wd[cols, :]).astype(BF16).astype(F32)
            act[:, cols] = (g * sigmoid(g) * u).astype(BF16)
            dgu[0, :, cols], dgu[1, :, cols] = silu_back(g, u, dact)

    row = lambda width: pl.BlockSpec((rows, width), lambda i: (i, 0))
    weight = once((None, d, ff), lambda i: (n, 0, 0))
    return Work(
        (t // rows,),
        [(a, row(d)), (dy, row(d)), (wg, weight), (wu, weight), (wd, once((None, ff, d), lambda i: (n, 0, 0)))],
        [((t, ff), BF16, row(ff)), ((2, t, ff), BF16, pl.BlockSpec((2, rows, ff), lambda i: (0, i, 0)))],
        body,
        6 * t * d * ff,
    )


def hidden_back(dh, wd, gate, up, n, rows):
    t, d = dh.shape
    ff = wd.shape[1]

    def body(dh, wd, gate, up, dgu):
        def piece(at, size):
            cols = pl.ds(at, size)
            dact = nt(dh[...], wd[cols, :]).astype(BF16).astype(F32)
            dgu[0, :, cols], dgu[1, :, cols] = silu_back(gate[:, cols], up[:, cols], dact)

        over_columns(ff, 1024, piece)

    row = lambda width: pl.BlockSpec((rows, width), lambda i: (i, 0))
    return Work(
        (t // rows,),
        [(dh, row(d)), (wd, once((None, ff, d), lambda i: (n, 0, 0))), (gate, row(ff)), (up, row(ff))],
        [((2, t, ff), BF16, pl.BlockSpec((2, rows, ff), lambda i: (0, i, 0)))],
        body,
        2 * t * d * ff,
    )


def input_back(dgu, wg, wu, h, dy, n, rows):
    _, t, ff = dgu.shape
    d = wg.shape[1]

    def body(dgu, wg, wu, h, dy, out, da):
        def piece(at, size):
            cols = pl.ds(at, size)
            da[:, cols] = nt(dgu[0], wg[cols, :]).astype(BF16) + nt(dgu[1], wu[cols, :]).astype(BF16)

        over_columns(d, 512, piece)
        out[...] = dy[...] + norm_back(h[...], da[...])

    row = lambda width: pl.BlockSpec((rows, width), lambda i: (i, 0))
    weight = once((None, d, ff), lambda i: (n, 0, 0))
    return Work(
        (t // rows,),
        [(dgu, pl.BlockSpec((2, rows, ff), lambda i: (0, i, 0))), (wg, weight), (wu, weight), (h, row(d)), (dy, row(d))],
        [((t, d), BF16, row(d)), ((t, d), BF16, row(d))],
        body,
        4 * t * d * ff,
    )


def by_down(act, dh, tile):
    t, ff = act.shape
    d = dh.shape[1]

    def body(act, dh, out):
        out[...] = tn(act[...], dh[...]).astype(BF16)

    return Work(
        (ff // tile,),
        [(act, pl.BlockSpec((t, tile), lambda i: (0, i))), (dh, once((t, d), lambda i: (0, 0)))],
        [((1, ff, d), BF16, pl.BlockSpec((None, tile, d), lambda i: (0, i, 0)))],
        body,
        2 * t * d * ff,
    )


def by_gate_up(a, dgu, tile, which):
    t, d = a.shape
    ff = dgu.shape[2]
    tiles, low = ff // tile, min(which)

    def body(a, dgu, out):
        out[...] = tn(dgu[...], a[...]).astype(BF16).T

    return Work(
        (len(which) * tiles,),
        [(a, once((t, d), lambda i: (0, 0))), (dgu, pl.BlockSpec((None, t, tile), lambda i: (low + i // tiles, 0, i % tiles)))],
        [((len(which), d, ff), BF16, pl.BlockSpec((None, d, tile), lambda i: (i // tiles, 0, i % tiles)))],
        body,
        2 * len(which) * t * d * ff,
    )


class Split:
    def __init__(self, rows, width, by_rows):
        self.rows, self.width, self.by_rows = rows, width, by_rows
        first = (width // 128 + 1) // 2 * 128
        self.colours = [(0, first), (first, width - first)]

    def part(self, colour, half):
        at, size = self.colours[colour]
        if self.by_rows:
            return pl.ds(half * (self.rows // 2), self.rows // 2), pl.ds(at, size)
        return pl.ds(0, self.rows), pl.ds(at + half * (size // 2), size // 2)

    def piece(self, colour):
        size = self.colours[colour][1]
        return (self.rows // 2, size) if self.by_rows else (self.rows, size // 2)

    def join(self, colours):
        along = 0 if self.by_rows else 1
        return jnp.concatenate([jnp.concatenate([c[0], c[1]], along) for c in colours], 1)


def position():
    me = lax.axis_index("dp")
    return lax.div(me, SIDE), lax.rem(me, SIDE)


def along(axis, at):
    x, y = position()
    return at * SIDE + y if axis == 0 else x * SIDE + at


def neighbours():
    x, y = position()
    for axis, here in ((0, x), (1, y)):
        for step in (1, SIDE - 1):
            yield along(axis, lax.rem(here + step, SIDE))


def over_blocks(out, f, *ins):
    def one(at, _):
        out[at] = f(*(i[at] for i in ins)).astype(out.dtype)
        return 0

    if len(out.shape) == 3:
        lax.fori_loop(0, out.shape[0], one, 0)
    else:
        one(Ellipsis, 0)


class Ring:
    def __init__(self, axis, source, own, scratch):
        self.axis, self.source, self.own = axis, source, own
        self.far, self.near, self.sums, self.terms, self.mine, self.send, self.recv, self.load = scratch
        here = position()[axis]
        self.here, self.right, self.left = here, lax.rem(here + 1, SIDE), lax.rem(here + SIDE - 1, SIDE)
        self.across = lax.rem(here + 2, SIDE)

    def message(self, i):
        src, dst = (
            (lambda: self.source(0, self.across), self.far.at[0]),
            (lambda: self.source(1, self.across), self.far.at[1]),
            (lambda: self.source(1, self.right), self.near.at[1]),
            (lambda: self.source(0, self.left), self.near.at[0]),
            (lambda: self.far.at[0], self.sums.at[0]),
            (lambda: self.far.at[1], self.sums.at[1]),
        )[i]
        to = self.right if i % 2 == 0 else self.left
        return pltpu.make_async_remote_copy(
            src_ref=src(),
            dst_ref=dst,
            send_sem=self.send.at[i],
            recv_sem=self.recv.at[i],
            device_id={"dp": along(self.axis, to)},
            device_id_type=MESH,
        )

    def local(self, i):
        src, dst = (
            (lambda: self.source(0, self.right), self.terms.at[0]),
            (lambda: self.source(1, self.left), self.terms.at[1]),
            (lambda: self.own(0), self.mine.at[0]),
            (lambda: self.own(1), self.mine.at[1]),
        )[i]
        return pltpu.make_async_copy(src(), dst, self.load.at[i])

    def start(self, first):
        for i in (0, 1) if first else (2, 3):
            self.message(i).start()

    def start_loads(self):
        for i in range(4):
            self.local(i).start()

    def relay(self):
        for half in (0, 1):
            self.local(half).wait()
            self.message(half).wait()
            over_blocks(self.far.at[half], lambda far, term: far.astype(F32) + term.astype(F32), self.far.at[half], self.terms.at[half])
            self.message(4 + half).start()

    def finish(self, take):
        for half in (0, 1):
            self.local(2 + half).wait()
        for i in (2, 3, 4, 5):
            self.message(i).wait()
        for half in (0, 1):
            take(half)


def ring_scratch(shape, own_type):
    return [
        pltpu.VMEM((2, *shape), BF16),
        pltpu.VMEM((2, *shape), BF16),
        pltpu.VMEM((2, *shape), BF16),
        pltpu.VMEM((2, *shape), BF16),
        pltpu.VMEM((2, *shape), own_type),
        pltpu.SemaphoreType.DMA((6,)),
        pltpu.SemaphoreType.DMA((6,)),
        pltpu.SemaphoreType.DMA((4,)),
    ]


RING_SCRATCH = 8


class First:
    def __init__(self, terms, which, split):
        self.term, self.which, self.split = terms, which, split

    def ins(self):
        return [(self.term, ANY)]

    def outs(self):
        made = []
        for colour in (0, 1):
            piece = self.split.piece(colour)
            for shape, kind in (((2, SIDE, *piece), BF16), ((2, *piece), F32)):
                made.append((shape, kind, pl.BlockSpec(shape, lambda i, n=len(shape): (0,) * n)))
        return made

    def scratch(self):
        return [s for colour in (0, 1) for s in ring_scratch((SIDE, *self.split.piece(colour)), BF16)]

    def rings(self, ins, outs, scratch):
        (term,) = ins
        made = []
        for colour in (0, 1):

            def source(half, at, colour=colour):
                rows, cols = self.split.part(colour, half)
                return term.at[self.which, at, :, rows, cols] if colour == 0 else term.at[self.which, :, at, rows, cols]

            axis = colour
            ring = Ring(axis, source, lambda half, s=source, axis=axis: s(half, position()[axis]), scratch[colour * RING_SCRATCH :][:RING_SCRATCH])
            made.append((ring, functools.partial(self.take, ring, outs[2 * colour], outs[2 * colour + 1], 1 - axis)))
        return made

    def take(self, ring, out, own, other, half):
        def total(*terms):
            return terms[0].astype(F32) + terms[1].astype(F32) + terms[2].astype(F32)

        refs = [r.at[half] for r in (ring.mine, ring.sums, ring.near)]
        over_blocks(out.at[half], total, *refs)
        own[half] = total(*(r[position()[other]] for r in refs))

    def after(self, ins, outs):
        pass


class Second:
    def __init__(self, parts, split, squares):
        self.squares = squares
        self.parts, self.split = parts, split

    def ins(self):
        return [(p, ANY) for p in self.parts] + [(self.squares, TILE)]

    def outs(self):
        shapes = [(2, *self.split.piece(colour)) for colour in (0, 1)]
        return [(shape, BF16, pl.BlockSpec(shape, lambda i: (0, 0, 0))) for shape in shapes] + [((8, 128), F32, TILE)]

    def scratch(self):
        return [s for colour in (0, 1) for s in ring_scratch(self.split.piece(colour), F32)]

    def rings(self, ins, outs, scratch):
        made = []
        for colour in (0, 1):
            part, own = ins[2 * colour : 2 * colour + 2]
            ring = Ring(
                1 - colour,
                lambda half, at, part=part: part.at[half, at],
                lambda half, own=own: own.at[half],
                scratch[colour * RING_SCRATCH :][:RING_SCRATCH],
            )
            made.append((ring, functools.partial(self.take, ring, outs[colour])))
        return made

    def take(self, ring, out, half):
        out[half] = (ring.mine[half] + ring.sums[half].astype(F32) + ring.near[half].astype(F32)).astype(BF16)

    def after(self, ins, outs):
        total = ins[4][...]
        for out in outs[:2]:
            for half in (0, 1):
                wide = out[half].astype(F32)
                total += jnp.sum(jnp.sum(wide * wide, 0, keepdims=True), 1, keepdims=True)
        outs[2][...] = total


class Clip:
    def __init__(self, members, count):
        self.members, self.count = members, count

    def ins(self):
        return []

    def outs(self):
        return [((8, 128), F32, TILE)]

    def scratch(self):
        sends = pltpu.SemaphoreType.DMA((self.members - 1,))
        return [pltpu.VMEM((8, 128), F32), pltpu.VMEM((self.members, 8, 128), F32), sends, sends]

    def peers(self):
        me = lax.axis_index("dp")
        return [lax.rem(me + i, self.members) for i in range(1, self.members)]

    def body(self, squares, factor, scratch):
        own, all_of_them, send, recv = scratch
        me = lax.axis_index("dp")
        own[...] = squares
        all_of_them[me] = squares

        def copy(i, slot):
            return pltpu.make_async_remote_copy(
                src_ref=own,
                dst_ref=all_of_them.at[slot],
                send_sem=send.at[i],
                recv_sem=recv.at[i],
                device_id={"dp": self.peers()[i]},
                device_id_type=MESH,
            )

        for i in range(self.members - 1):
            copy(i, me).start()
        for i in range(self.members - 1):
            copy(i, me).wait_send()
            copy(i, lax.rem(me + self.members - 1 - i, self.members)).wait_recv()
        total = all_of_them[0]
        for member in range(1, self.members):
            total += all_of_them[member]
        factor[...] = jnp.minimum(1.0, 0.5 * lax.rsqrt(total / self.count + 1e-30))


def run(work=None, first=None, second=None, name=None, number=None, relay=(0.3, 0.5), clip=None):
    parts = [p for p in (second, first) if p is not None]
    grid = work.grid if work else (1,)
    steps = grid[0]
    groups = ([work] if work else []) + parts
    ins = [list(work.ins)] if work else []
    ins += [p.ins() for p in parts]
    outs = [list(work.outs)] if work else []
    outs += [p.outs() for p in parts]
    scratch = [p.scratch() for p in parts]
    if clip:
        outs.append(clip.outs())
        scratch.append(clip.scratch())

    def cut(refs, sizes):
        made = []
        for size in sizes:
            made.append(refs[:size])
            refs = refs[size:]
        return made

    n_in, n_out = sum(map(len, ins)), sum(map(len, outs))

    def kernel(*refs):
        in_refs = cut(refs[:n_in], [len(i) for i in ins])
        out_refs = cut(refs[n_in : n_in + n_out], [len(o) for o in outs])
        scratch_refs = cut(refs[n_in + n_out :], [len(s) for s in scratch])
        step = pl.program_id(0)
        skip = 1 if work else 0
        rings = [p.rings(in_refs[skip + i], out_refs[skip + i], scratch_refs[i]) for i, p in enumerate(parts)]
        if parts:

            @pl.when(step == 0)
            def _():
                barrier = pltpu.get_barrier_semaphore()
                greeted = clip.peers() if clip else list(neighbours())
                for device in greeted:
                    pl.semaphore_signal(barrier, inc=1, device_id={"dp": device}, device_id_type=MESH)
                pl.semaphore_wait(barrier, len(greeted))
                for first_ones in (True, False):
                    for group in rings:
                        for ring, _ in group:
                            ring.start(first_ones)
                for group in rings:
                    for ring, _ in group:
                        ring.start_loads()

            for i, group in enumerate(rings):
                at = int(steps * (relay[i] if len(rings) == 2 else relay[1]))

                @pl.when(step == at)
                def _():
                    for ring, _ in group:
                        ring.relay()

        if work:
            work.body(*in_refs[0], *out_refs[0])
        if parts:

            @pl.when(step == steps - 1)
            def _():
                for group in rings:
                    for ring, take in group:
                        ring.finish(take)
                for i, part in enumerate(parts):
                    part.after(in_refs[skip + i], out_refs[skip + i])
                if clip:
                    clip.body(out_refs[skip][2][...], out_refs[-1][0], scratch_refs[-1])

    made = pl.pallas_call(
        kernel,
        out_shape=[jax.ShapeDtypeStruct(shape, kind) for group in outs for shape, kind, _ in group],
        grid_spec=pltpu.PrefetchScalarGridSpec(
            num_scalar_prefetch=0,
            grid=grid,
            in_specs=[spec for group in ins for _, spec in group],
            out_specs=[spec for group in outs for _, _, spec in group],
            scratch_shapes=[s for group in scratch for s in group],
        ),
        compiler_params=pltpu.CompilerParams(
            dimension_semantics=("arbitrary",),
            vmem_limit_bytes=VMEM_LIMIT,
            **(dict(collective_id=number, has_side_effects=True) if parts else {}),
        ),
        cost_estimate=pl.CostEstimate(flops=work.flops if work else 1000, bytes_accessed=1 << 24, transcendentals=0),
        name=name,
    )(*[a for group in ins for a, _ in group])
    return cut(made, [len(o) for o in outs])


class Spread:
    def __init__(self, block, out, split, colour, send, recv):
        self.block, self.out, self.split, self.colour, self.send, self.recv = block, out, split, colour, send, recv

    def region(self, stage, half, place):
        rows, cols = self.split.part(self.colour, half)
        x, y = position()
        if stage == 0:
            x, y = (place, y) if self.colour == 0 else (x, place)
            return self.out.at[:, x, y, rows, cols]
        return self.out.at[:, :, place, rows, cols] if self.colour == 0 else self.out.at[:, place, :, rows, cols]

    def message(self, stage, i, arriving=False):
        axis = self.colour if stage == 0 else 1 - self.colour
        here = position()[axis]
        right, left = lax.rem(here + 1, SIDE), lax.rem(here + SIDE - 1, SIDE)
        sender = here if not arriving else (left if i % 2 == 0 else right)
        half = (0, 1, 1, 0, 0, 1)[i]
        owner = sender if i < 4 else lax.rem(sender + (SIDE - 1 if i == 4 else 1), SIDE)
        region = self.region(stage, half, owner)
        src = region
        if stage == 0 and i < 4:
            rows, cols = self.split.part(self.colour, half)
            src = self.block.at[:, rows, cols]
        return pltpu.make_async_remote_copy(
            src_ref=src,
            dst_ref=region,
            send_sem=self.send.at[stage, i],
            recv_sem=self.recv.at[stage, i],
            device_id={"dp": along(axis, right if i % 2 == 0 else left)},
            device_id_type=MESH,
        )

    def start(self, stage, first):
        for i in (0, 1) if first else (2, 3):
            self.message(stage, i).start()

    def hand_on(self, stage):
        for i in (0, 1):
            self.message(stage, i, True).wait_recv()
            self.message(stage, 4 + i).start()

    def arrived(self, stage):
        for i in (2, 3, 4, 5):
            self.message(stage, i, True).wait_recv()

    def sent(self):
        for stage in (0, 1):
            for i in range(6):
                self.message(stage, i).wait_send()


def gathered(blocks, splits, number):
    n = len(blocks)

    def kernel(*refs):
        ins, outs, held = refs[:n], refs[n : 2 * n], refs[2 * n : 3 * n]
        send, recv, load, store = refs[3 * n :]
        spreads = [[Spread(ins[k], outs[k], splits[k], c, send.at[k, c], recv.at[k, c]) for c in (0, 1)] for k in range(n)]
        x, y = position()
        loads = [lambda k=k: pltpu.make_async_copy(ins[k], held[k], load.at[k]) for k in range(n)]
        stores = [lambda k=k: pltpu.make_async_copy(held[k], outs[k].at[:, x, y], store.at[k]) for k in range(n)]
        for k in range(n):
            loads[k]().start()
        barrier = pltpu.get_barrier_semaphore()
        for device in neighbours():
            pl.semaphore_signal(barrier, inc=1, device_id={"dp": device}, device_id_type=MESH)
        pl.semaphore_wait(barrier, 4)
        for k in range(n):
            for first in (True, False):
                for spread in spreads[k]:
                    spread.start(0, first)
        for k in range(n):
            loads[k]().wait()
            stores[k]().start()
        for k in range(n):
            for spread in spreads[k]:
                spread.hand_on(0)
        for k in range(n):
            stores[k]().wait()
            for spread in spreads[k]:
                spread.arrived(0)
            for first in (True, False):
                for spread in spreads[k]:
                    spread.start(1, first)
        for k in range(n):
            for spread in spreads[k]:
                spread.hand_on(1)
        for k in range(n):
            for spread in spreads[k]:
                spread.arrived(1)
                spread.sent()

    return pl.pallas_call(
        kernel,
        out_shape=[jax.ShapeDtypeStruct((b.shape[0], SIDE, SIDE, *b.shape[1:]), b.dtype) for b in blocks],
        in_specs=[ANY] * n,
        out_specs=[ANY] * n,
        scratch_shapes=[pltpu.VMEM(b.shape, b.dtype) for b in blocks]
        + [pltpu.SemaphoreType.DMA((n, 2, 2, 6)), pltpu.SemaphoreType.DMA((n, 2, 2, 6)), pltpu.SemaphoreType.DMA((n,)), pltpu.SemaphoreType.DMA((n,))],
        compiler_params=pltpu.CompilerParams(collective_id=number, has_side_effects=True, vmem_limit_bytes=VMEM_LIMIT),
        name="gathered",
    )(*blocks)


def adamw(w, m, v, g):
    m = 0.9 * m + 0.1 * g
    v = 0.95 * v + 0.05 * g * g
    step = m * lax.rsqrt(v + 1e-8) + 0.1 * w
    return (w - 0.02 * step).astype(BF16), m, v


def solution(mesh):
    members = mesh.shape["dp"]

    def step(x, dy, wg, wu, wd, *moments):
        x, dy = x[0], dy[0]
        d, ff = wg.shape[1:]
        wide, tall = Split(d // members, ff, True), Split(ff // members, d, False)
        square = lambda t: t.reshape(t.shape[0], SIDE, SIDE, t.shape[1] // members, t.shape[2])

        none = jnp.zeros((8, 128), F32)
        [[gate0, up0, act0, a0]] = run(gate_up(x, wg, wu, 0, 256), name="gate_up_0")
        [[h1, a1]] = run(down(act0, wd, x, 0, 256), name="down_0")
        [[act1, dgu1]] = run(last_layer(a1, dy, wg, wu, wd, 1, 256), name="layer_1")
        [[d1]] = run(by_down(act1, dy, 640), name="by_down_1")
        [[gu1], d1_half] = run(by_gate_up(a1, dgu1, 640, (0, 1)), First(square(d1), 0, tall), name="by_gate_up_1", number=1)
        gu1 = square(gu1)
        [[dh1, _], [*d1_sum, squares], g1_half] = run(
            input_back(dgu1, wg, wu, h1, dy, 1, 256), First(gu1, 0, wide), Second(d1_half, tall, none), name="input_back_1", number=2
        )
        [[dgu0], [*g1_sum, squares], u1_half] = run(
            hidden_back(dh1, wd, gate0, up0, 0, 256), First(gu1, 1, wide), Second(g1_half, wide, squares), name="hidden_back_0", number=3
        )
        [[d0], [*u1_sum, squares]] = run(by_down(act0, dh1, 640), None, Second(u1_half, wide, squares), name="by_down_0", number=4)
        [[g0], d0_half] = run(by_gate_up(a0, dgu0, 640, (0,)), First(square(d0), 0, tall), name="by_gate_0", number=5, relay=(0.6, 0.8))
        [[u0], [*d0_sum, squares], g0_half] = run(
            by_gate_up(a0, dgu0, 640, (1,)),
            First(square(g0), 0, wide),
            Second(d0_half, tall, squares),
            name="by_up_0",
            number=6,
            relay=(0.6, 0.8),
        )
        [[*g0_sum, squares], u0_half] = run(None, First(square(u0), 0, wide), Second(g0_half, wide, squares), name="sum_up_0", number=7)
        count = sum(w.size for w in (wg, wu, wd))
        [[*u0_sum, _], [factor]] = run(None, None, Second(u0_half, wide, squares), name="sum_end", number=8, clip=Clip(members, count))
        factor = factor[0, 0]

        g = [
            jnp.stack([split.join(one) for one in sums]).astype(F32)
            for split, sums in ((wide, (g0_sum, g1_sum)), (wide, (u0_sum, u1_sum)), (tall, (d0_sum, d1_sum)))
        ]
        me = lax.axis_index("dp")
        new = []
        for w, m, v, one in zip((wg, wu, wd), moments[:3], moments[3:], g, strict=True):
            rows = w.shape[1] // members
            mine = lax.dynamic_slice_in_dim(w, me * rows, rows, 1).astype(F32)
            new.append(adamw(mine, m, v, one * factor))
        weights = gathered([w for w, _, _ in new], (wide, wide, tall), 10)
        weights = [one.reshape(w.shape) for one, w in zip(weights, (wg, wu, wd), strict=True)]
        return (*weights, *(m for _, m, _ in new), *(v for _, _, v in new))

    parts, whole, moment, out = P(("rep", "dp"), None, None), P(None, None, None), P(None, "dp", None), P("rep", "dp", None)
    return jax.shard_map(
        step,
        mesh=mesh,
        in_specs=(parts,) * 2 + (whole,) * 3 + (moment,) * 6,
        out_specs=(P("rep", None, None),) * 3 + (out,) * 6,
        check_vma=False,
    )
```
